32 devices in a mesh: mem: 8 (over z, x), blk: 4 (over y, core).
Axes of the slice: x: 2, y: 2, z: 4, core: 2. Of those that a mesh axis runs over, the one named last changes fastest.
Arguments:
- ensemble: bfloat16 [128, 131072], P('mem', 'blk'), may hold values from -6 to 6
- obs_cell: int32 [4, 64, 256], P('blk', 'mem'), may hold values from 0 to 511
- obs_count: int32 [4, 64], P('blk', 'mem'), may hold values from 1 to 256, 10240 in all within a row
- obs_value: float32 [4, 64, 256], P('blk', 'mem'), may hold values from -6 to 6
- obs_rinv: float32 [4, 64, 256], P('blk', 'mem'), may hold values from 0.05 to 0.5
Outputs:
- increments: bfloat16 [128, 131072], P('mem', 'blk')
The draws below stay inside these ranges and needn't reach their ends.
Inputs may be any that keep to these rules, and one draw needn't show every extreme that they name: `obs_cell`: slots at or past the block's count are unused. `obs_count`: the counts of one band sum to 10240, and some block holds exactly 256.
All inputs are finite; a program needn't handle non-finite values. Where the reference program divides by a largest or mean magnitude, that divisor is 1e-20 or more.
Results may differ from the reference program's by a relative error of at most 0.0051.
Values may be sent and summed in bfloat16 or wider, within the bound.
A program may use at most 64 MiB of HBM per device.

```python
import math
import jax
import jax.numpy as jnp
import numpy as np
from jax import lax

K = 128
CELLS = 512
OMAX = 256
NS_ITERS = 4
NSB = 64
CELLS_ALL = 131072
N_BLK = 4


def place_ends(array, key, least, top_value):
    shape = array.shape
    index_at = [jax.random.randint(jax.random.fold_in(key, axis), (), 0, shape[axis]) for axis in range(len(shape))]
    array = array.at[tuple(index_at)].set(least)
    longest = shape.index(max(shape))
    index_at[longest] = (index_at[longest] + 1) % shape[longest]
    return array.at[tuple(index_at)].set(top_value)


def block_scale(key, dims, pieces, smallest, largest):
    loudness, own = 1.0, jax.random.fold_in(key, 6)
    for dim, blocks in pieces:
        draws = jnp.exp(jax.random.uniform(jax.random.fold_in(own, dim), (blocks,), jnp.float32, smallest / len(pieces), largest / len(pieces)))
        loudness = loudness * jnp.repeat(draws, dims[dim] // blocks).reshape([-1 if axis == dim else 1 for axis in range(len(dims))])
    return loudness


def length_profile(count, total, limit, lean):
    portions = [(1 << 20) // math.isqrt(grade ** lean) + 1 for grade in range(2, count + 1)]
    rest, counts = total - limit - (count - 1), [1] * (count - 1)
    while rest > 0:
        movable = [i for i in range(count - 1) if counts[i] < limit]
        mass, remaining = sum([portions[i] for i in movable]), rest
        for i in movable:
            extra = min(limit - counts[i], max(1, remaining * portions[i] // mass), rest)
            counts[i] = counts[i] + extra
            rest = rest - extra
    return np.array([limit] + counts)


def uneven(stream_key, count, total, most, lean):
    if count == 2:
        one = jax.random.randint(stream_key, (), max(1, total - most), min(most, total - 1) + 1)
        return jnp.stack([one, total - one])
    sizes = jnp.asarray(length_profile(count, total, most, lean), jnp.int32)
    pairs = (count - 1) // 2
    giver, receiver = sizes[1:1 + 2 * pairs:2], sizes[2:2 + 2 * pairs:2]
    margin = jnp.minimum(giver - 1, most - receiver)
    passed = jax.random.randint(jax.random.fold_in(stream_key, 1), (pairs,), 0, 1 << 20) % (margin + 1)
    sizes = sizes.at[1:1 + 2 * pairs:2].set(giver - passed).at[2:2 + 2 * pairs:2].set(receiver + passed)
    return sizes[jax.random.permutation(jax.random.fold_in(stream_key, 2), count)]


def bell_draw(own_key, shape, scale, bound, split=(), kind=jnp.bfloat16):
    array = jax.random.normal(own_key, shape, jnp.float32) * scale
    if len(split) > 0:
        array = block_scale(own_key, shape, split, -0.22, 0.18) * array
    return jnp.clip(array, min=-bound, max=bound).astype(kind)


def setup_inputs(seed: int = 0) -> dict:
    seeds = jax.random.split(jax.random.key(seed), 6)
    ensemble = bell_draw(seeds[0], (K, CELLS_ALL), 1.0, 6.0, ((0, 8), (1, 4)))
    obs_cell = place_ends(jax.random.randint(seeds[1], (N_BLK, NSB, OMAX), 0, CELLS), jax.random.fold_in(seeds[1], 1), 0, CELLS - 1).astype(jnp.int32)
    obs_count = jax.vmap(lambda own: uneven(own, NSB, NSB * OMAX * 5 // 8, OMAX, 2))(jax.random.split(seeds[2], N_BLK)).reshape((N_BLK, NSB)).astype(jnp.int32)
    obs_value = bell_draw(seeds[3], (N_BLK, NSB, OMAX), 1.0, 6.0, ((0, 4), (1, 8)), jnp.float32)
    obs_rinv = jnp.clip(jnp.exp(math.log(0.5) - 2.3025851 * jax.random.uniform(seeds[4], (N_BLK, NSB, OMAX), jnp.float32) ** block_scale(seeds[4], (N_BLK, NSB, OMAX), ((0, 4), (1, 8)), -0.2, 0.2)), 0.05, 0.5)
    return {"ensemble": ensemble, "obs_cell": obs_cell, "obs_count": obs_count, "obs_value": obs_value, "obs_rinv": obs_rinv}


localize = 0.5
inflation = 1.1

def center(members):
    values = members.astype(jnp.float32)
    average = lax.optimization_barrier(jnp.mean(values, axis=0))
    return (values - average[None], average)

def observe(deviation, average, cell_ids, live_counts, obs_values, inv_var):
    ensemble_size = deviation.shape[0]
    index = jnp.broadcast_to(cell_ids[None].astype(jnp.int32), (ensemble_size,) + cell_ids.shape)
    sampled = jnp.take_along_axis(deviation, index, axis=2)
    obs_mean = jnp.take_along_axis(average, cell_ids.astype(jnp.int32), axis=1)
    slots = lax.broadcasted_iota(jnp.int32, cell_ids.shape, 1)
    live = (slots < live_counts[:, None].astype(jnp.int32)).astype(jnp.float32)
    weight_root = live * jnp.sqrt(inv_var)
    upper = jnp.transpose(sampled * weight_root[None], (1, 0, 2))
    lower = (weight_root * (obs_values - obs_mean))[:, None, :]
    return jnp.concatenate([upper, lower], axis=1).astype(jnp.bfloat16)

def batch_mm(left, right):
    return jnp.einsum('bij,bjk->bik', left, right, precision=lax.Precision.HIGHEST)

def transform_apply(localized, deviation):
    ensemble_size = deviation.shape[0]
    identity = jnp.eye(ensemble_size, dtype=jnp.float32)
    system = (ensemble_size - 1) / inflation * identity + localized[:, :ensemble_size, :ensemble_size]
    forcing = localized[:, :ensemble_size, ensemble_size]
    bound_norm = lax.optimization_barrier(jnp.max(lax.optimization_barrier(jnp.sum(jnp.abs(system), axis=2)), axis=1))
    approx_y = system / bound_norm[:, None, None]
    approx_z = jnp.broadcast_to(identity, system.shape)
    for iteration in range(NS_ITERS):
        update = 1.5 * identity - 0.5 * batch_mm(approx_z, approx_y)
        approx_y = batch_mm(approx_y, update)
        approx_z = batch_mm(update, approx_z)
    root_inv = approx_z / jnp.sqrt(bound_norm)[:, None, None]
    inner = jnp.einsum('bij,bj->bi', root_inv, forcing, precision=lax.Precision.HIGHEST)
    mean_weights = jnp.einsum('bij,bj->bi', root_inv, inner, precision=lax.Precision.HIGHEST)
    mixing = jnp.sqrt(jnp.float32(ensemble_size - 1)) * root_inv + mean_weights[:, :, None] - identity
    increment = jnp.einsum('jbc,bjk->kbc', deviation, mixing, precision=lax.Precision.HIGHEST)
    return increment.astype(jnp.bfloat16)

def reference(ensemble, obs_cell, obs_count, obs_value, obs_rinv):
    bands = obs_cell.shape[0]
    sectors = obs_cell.shape[1]
    grid = jnp.transpose(ensemble.reshape(K, bands, sectors, CELLS), (1, 0, 2, 3))

    def one_band(band_inputs):
        members, cell_ids, live_counts, obs_values, inv_var = band_inputs
        deviation, average = center(members)
        obs_rows = observe(deviation, average, cell_ids, live_counts, obs_values, inv_var)
        wide_rows = obs_rows.astype(jnp.float32)
        gram_blocks = jnp.einsum('bko,bjo->bkj', wide_rows, wide_rows, precision=lax.Precision.HIGHEST)
        localized = gram_blocks + localize * (jnp.roll(gram_blocks, 1, axis=0) + jnp.roll(gram_blocks, -1, axis=0))
        return transform_apply(localized, deviation)
    result = lax.map(one_band, (grid, obs_cell, obs_count, obs_value, obs_rinv))
    return jnp.transpose(result, (1, 0, 2, 3)).reshape(K, bands * sectors * CELLS)
```

```python
import functools

import jax
import jax.numpy as jnp
from jax import lax
from jax.experimental import pallas as pl
from jax.experimental.pallas import tpu as pltpu
from jax.sharding import PartitionSpec as P

NS_ITERS = 4


localize = 0.5
inflation = 1.1

MESH = pl.DeviceIdType.MESH
F32 = jnp.float32
BF16 = jnp.bfloat16


def halves(x):
    high = x.astype(BF16)
    return high, (x - high.astype(F32)).astype(BF16)


def as_left(x):
    return jnp.concatenate(halves(x), axis=1)


def as_right(x):
    wide = jnp.concatenate(halves(x), axis=1)
    return jnp.concatenate([wide, wide], axis=0)


def mm(left, right):
    both = jnp.dot(left, right, preferred_element_type=F32)
    size = both.shape[1] // 2
    return both[:, :size] + both[:, size:]


def observed_rows(members, selector, values, root):
    ensemble_size = members.shape[0]
    sampled = jnp.dot(members, selector, preferred_element_type=F32)
    obs_mean = jnp.sum(sampled, axis=0, keepdims=True) * (1.0 / ensemble_size)
    upper = ((sampled - obs_mean) * root).astype(BF16)
    lower = root * (values - obs_mean)
    place = lax.broadcasted_iota(jnp.int32, (16, lower.shape[1]), 0)
    lower = jnp.where(place == 0, jnp.broadcast_to(lower, place.shape), 0.0).astype(BF16)
    return jnp.concatenate([upper, lower], axis=0)


def increments_of(localized, members):
    ensemble_size = members.shape[0]
    row = lax.broadcasted_iota(jnp.int32, (ensemble_size, ensemble_size), 0)
    column = lax.broadcasted_iota(jnp.int32, (ensemble_size, ensemble_size), 1)
    identity = (row == column).astype(F32)
    system = (ensemble_size - 1) / inflation * identity + localized[:ensemble_size]
    bound_norm = jnp.max(
        jnp.sum(jnp.abs(system), axis=0, keepdims=True), axis=1, keepdims=True
    )
    approx_y = system / bound_norm
    update = 1.5 * identity - 0.5 * approx_y
    approx_z = update
    for iteration in range(1, NS_ITERS):
        approx_y = mm(as_left(approx_y), as_right(update))
        left_z = as_left(approx_z)
        update = 1.5 * identity - 0.5 * mm(left_z, as_right(approx_y))
        approx_z = mm(left_z, as_right(update))
    root_inv = approx_z / jnp.sqrt(bound_norm)
    right_r = as_right(root_inv)
    inner = mm(as_left(localized[ensemble_size:]), right_r)
    mean_weights = mm(as_left(inner), right_r)[0:1]
    mixing = jnp.sqrt(F32(ensemble_size - 1)) * root_inv + mean_weights - identity
    high, low = halves(mixing)
    row_sum = jnp.sum(high.astype(F32) + low.astype(F32), axis=1, keepdims=True)
    average = jnp.sum(members.astype(F32), axis=0, keepdims=True) * (1.0 / ensemble_size)
    total = jnp.dot(
        jnp.concatenate([high, low], axis=1),
        jnp.concatenate([members, members], axis=0),
        preferred_element_type=F32,
    )
    return (total - row_sum * average).astype(BF16)


def kernel(
    groups,
    ens,
    cell,
    count,
    value,
    rinv,
    out,
    arrived,
    rows,
    gram,
    selector,
    stage,
    weight,
    own_sem,
    fwd_send,
    fwd_recv,
    ret_send,
    ret_recv,
    halo_send,
    halo_recv,
):
    me = lax.axis_index("mem")
    blocks, _, width = arrived.shape
    local = ens.shape[0]
    slots = cell.shape[1]
    size = groups * local

    barrier = pltpu.get_barrier_semaphore()
    for step in range(1, groups):
        pl.semaphore_signal(
            barrier, inc=1, device_id={"mem": lax.rem(me + step, groups)}, device_id_type=MESH
        )

    weight[...] = jnp.sqrt(rinv[...])

    @pl.loop(0, blocks)
    def _(b):
        positions = lax.broadcasted_iota(jnp.int32, (width, slots), 0)
        selector[b] = jnp.where(positions == cell[pl.ds(b, 1), :], 1.0, 0.0).astype(BF16)

    pl.semaphore_wait(barrier, groups - 1)

    def columns(owner, b):
        start = pl.multiple_of((owner * blocks + b) * width, width)
        return pl.ds(start, width)

    def members_of(owner):
        return pl.ds(pl.multiple_of(owner * local, local), local)

    @pl.loop(0, blocks)
    def _(i):
        b = lax.rem(i + blocks - 1, blocks)
        for step in range(1, groups):
            peer = lax.rem(me + step, groups)
            pltpu.make_async_remote_copy(
                src_ref=ens.at[:, columns(peer, b)],
                dst_ref=arrived.at[b, members_of(me), :],
                send_sem=fwd_send,
                recv_sem=fwd_recv.at[b],
                device_id={"mem": peer},
                device_id_type=MESH,
            ).start()
        pltpu.make_async_copy(
            ens.at[:, columns(me, b)], arrived.at[b, members_of(me), :], fwd_recv.at[b]
        ).start()

    def form_gram(slot):
        held = rows[slot]
        gram[slot] = lax.dot_general(
            held, held[:size], (((1,), (1,)), ((), ())), preferred_element_type=F32
        )

    def take_block(b):
        pltpu.make_async_copy(arrived.at[b], arrived.at[b], fwd_recv.at[b]).wait()
        alive = lax.broadcasted_iota(jnp.int32, (1, slots), 1) < count[0, b]
        root = jnp.where(alive, weight[pl.ds(b, 1), :], 0.0)
        rows[b + 1] = observed_rows(arrived[b], selector[b], value[pl.ds(b, 1), :], root)

    def give_block(b):
        localized = gram[b + 1] + localize * (gram[b] + gram[b + 2])
        stage[b] = increments_of(localized, arrived[b])
        for step in range(1, groups):
            peer = lax.rem(me + step, groups)
            pltpu.make_async_remote_copy(
                src_ref=stage.at[b, members_of(peer), :],
                dst_ref=out.at[:, columns(me, b)],
                send_sem=ret_send,
                recv_sem=ret_recv,
                device_id={"mem": peer},
                device_id_type=MESH,
            ).start()
        pltpu.make_async_copy(
            stage.at[b, members_of(me), :], out.at[:, columns(me, b)], own_sem
        ).start()

    def halo(source, target, peer, which):
        return pltpu.make_async_remote_copy(
            src_ref=rows.at[source],
            dst_ref=rows.at[target],
            send_sem=halo_send.at[which],
            recv_sem=halo_recv.at[which],
            device_id={"mem": peer},
            device_id_type=MESH,
        )

    upward = halo(blocks, 0, lax.rem(me + 1, groups), 0)
    downward = halo(1, blocks + 1, lax.rem(me + groups - 1, groups), 1)

    take_block(blocks - 1)
    upward.start()
    form_gram(blocks)
    take_block(0)
    downward.start()
    form_gram(1)
    take_block(1)
    form_gram(2)
    upward.wait_recv()
    form_gram(0)
    give_block(0)

    @pl.loop(2, blocks - 1)
    def _(b):
        take_block(b)
        form_gram(b + 1)
        give_block(b - 1)

    downward.wait_recv()
    form_gram(blocks + 1)

    @pl.loop(blocks - 2, blocks)
    def _(b):
        give_block(b)

    upward.wait_send()
    downward.wait_send()
    share = blocks * width
    afar = pl.ds(0, (groups - 1) * share)
    pltpu.make_async_copy(ens.at[:, afar], ens.at[:, afar], fwd_send).wait()
    pltpu.make_async_copy(out.at[:, afar], out.at[:, afar], ret_send).wait()
    pltpu.make_async_copy(out.at[:, afar], out.at[:, afar], ret_recv).wait()
    near = pl.ds(0, share)
    pltpu.make_async_copy(out.at[:, near], out.at[:, near], own_sem).wait()


def fused(ensemble, obs_cell, obs_count, obs_value, obs_rinv):
    groups = lax.axis_size("mem")
    local, cells = ensemble.shape
    blocks, slots = obs_cell.shape[1:]
    width = cells // (groups * blocks)
    size = groups * local
    whole = pl.BlockSpec(memory_space=pltpu.VMEM)
    return pl.pallas_call(
        functools.partial(kernel, groups),
        out_shape=jax.ShapeDtypeStruct(ensemble.shape, BF16),
        in_specs=[whole, whole, pl.BlockSpec(memory_space=pltpu.SMEM), whole, whole],
        out_specs=whole,
        scratch_shapes=[
            pltpu.VMEM((blocks, size, width), BF16),
            pltpu.VMEM((blocks + 2, size + 16, slots), BF16),
            pltpu.VMEM((blocks + 2, size + 16, size), F32),
            pltpu.VMEM((blocks, width, slots), BF16),
            pltpu.VMEM((blocks, size, width), BF16),
            pltpu.VMEM((blocks, slots), F32),
            pltpu.SemaphoreType.DMA,
            pltpu.SemaphoreType.DMA,
            pltpu.SemaphoreType.DMA((blocks,)),
            pltpu.SemaphoreType.DMA,
            pltpu.SemaphoreType.DMA,
            pltpu.SemaphoreType.DMA((2,)),
            pltpu.SemaphoreType.DMA((2,)),
        ],
        compiler_params=pltpu.CompilerParams(collective_id=0, has_side_effects=True),
        name="letkf",
    )(ensemble, obs_cell[0], obs_count, obs_value[0], obs_rinv[0])


def with_halo(block, sides, width):
    for axis, dim in sides:
        count = lax.axis_size(axis)
        forward = [(i, i + 1) for i in range(count - 1)]
        forward.append((count - 1, 0))
        backward = [(target, source) for source, target in forward]
        low = lax.ppermute(
            lax.slice_in_dim(block, block.shape[dim] - width, None, axis=dim), axis, forward
        )
        high = lax.ppermute(lax.slice_in_dim(block, 0, width, axis=dim), axis, backward)
        block = jnp.concatenate([low, block, high], axis=dim)
    return block


def center_blocks(members):
    values = jnp.transpose(members.astype(jnp.float32), (1, 0, 2))
    average = jnp.mean(values, axis=1)
    return (values - average[:, None, :], average)


def observe(deviation, average, cell_ids, live_counts, obs_values, inv_var):
    cell_width = deviation.shape[2]
    positions = lax.broadcasted_iota(jnp.int32, cell_ids.shape + (cell_width,), 2)
    selector = (positions == cell_ids[:, :, None]).astype(jnp.float32)
    sampled = jnp.einsum("bkc,boc->bko", deviation, selector, precision=lax.Precision.HIGHEST)
    obs_mean = jnp.einsum("bc,boc->bo", average, selector, precision=lax.Precision.HIGHEST)
    slots = lax.broadcasted_iota(jnp.int32, cell_ids.shape, 1)
    live = (slots < live_counts[:, None]).astype(jnp.float32)
    weight_root = live * jnp.sqrt(inv_var)
    upper = sampled * weight_root[:, None, :]
    lower = (weight_root * (obs_values - obs_mean))[:, None, :]
    return jnp.concatenate([upper, lower], axis=1).astype(jnp.bfloat16)


def gram_of(obs_rows):
    return jnp.einsum("bko,bjo->bkj", obs_rows, obs_rows, preferred_element_type=jnp.float32)


def batch_mm(left, right):
    return jnp.einsum("bij,bjk->bik", left, right, precision=lax.Precision.HIGHEST)


def transform_apply(localized, deviation):
    ensemble_size = deviation.shape[1]
    identity = jnp.eye(ensemble_size, dtype=jnp.float32)
    system = (ensemble_size - 1) / inflation * identity + localized[
        :, :ensemble_size, :ensemble_size
    ]
    forcing = localized[:, :ensemble_size, ensemble_size]
    bound_norm = jnp.max(jnp.sum(jnp.abs(system), axis=2), axis=1)
    approx_y = system / bound_norm[:, None, None]
    approx_z = jnp.broadcast_to(identity, system.shape)
    for iteration in range(NS_ITERS):
        update = 1.5 * identity - 0.5 * batch_mm(approx_z, approx_y)
        approx_y = batch_mm(approx_y, update)
        approx_z = batch_mm(update, approx_z)
    root_inv = approx_z / jnp.sqrt(bound_norm)[:, None, None]
    inner = jnp.einsum("bij,bj->bi", root_inv, forcing, precision=lax.Precision.HIGHEST)
    mean_weights = jnp.einsum("bij,bj->bi", root_inv, inner, precision=lax.Precision.HIGHEST)
    mixing = (
        jnp.sqrt(jnp.float32(ensemble_size - 1)) * root_inv + mean_weights[:, :, None] - identity
    )
    increment = jnp.einsum("bjc,bjk->kbc", deviation, mixing, precision=lax.Precision.HIGHEST)
    return increment.astype(jnp.bfloat16)


def on_device(ensemble, obs_cell, obs_count, obs_value, obs_rinv):
    groups = lax.axis_size("mem")
    local_members = ensemble.shape[0]
    blocks = obs_cell.shape[1]
    cell_width = ensemble.shape[1] // (groups * blocks)
    pieces = ensemble.reshape(local_members, groups, blocks, cell_width)
    arrived = lax.all_to_all(pieces, "mem", split_axis=1, concat_axis=0, tiled=True)
    deviation, average = center_blocks(arrived[:, 0])
    obs_rows = observe(deviation, average, obs_cell[0], obs_count[0], obs_value[0], obs_rinv[0])
    padded_rows = with_halo(obs_rows, (("mem", 0),), 1)
    padded = gram_of(padded_rows)
    localized = padded[1:-1] + localize * (padded[:-2] + padded[2:])
    increment = transform_apply(localized, deviation)
    ensemble_size = increment.shape[0]
    outgoing = increment.reshape(ensemble_size, 1, blocks * cell_width)
    returned = lax.all_to_all(outgoing, "mem", split_axis=0, concat_axis=1, tiled=True)
    return returned.reshape(local_members, groups * blocks * cell_width)


def by_shape(ensemble, *observations):
    groups = lax.axis_size("mem")
    local, cells = ensemble.shape
    blocks, slots = observations[0].shape[1:]
    width = cells // (groups * blocks)
    aligned = local % 16 == 0 and width % 128 == 0 and slots % 128 == 0
    aligned = aligned and (groups * local) % 128 == 0 and groups > 1 and blocks > 2
    return (fused if aligned else on_device)(ensemble, *observations)


def solution(mesh):
    placed = (
        P("mem", "blk"),
        P("blk", "mem", None),
        P("blk", "mem"),
        P("blk", "mem", None),
        P("blk", "mem", None),
    )
    return jax.shard_map(
        by_shape, mesh=mesh, in_specs=placed, out_specs=P("mem", "blk"), check_vma=False
    )
```

```python
import functools

import jax
import jax.numpy as jnp
from jax import lax
from jax.experimental import pallas as pl
from jax.experimental.pallas import tpu as pltpu
from jax.sharding import PartitionSpec as P

NS_ITERS = 4


localize = 0.5
inflation = 1.1

MESH = pl.DeviceIdType.MESH
WINDOW = 3
F32 = jnp.float32
BF16 = jnp.bfloat16


def halves(x):
    high = x.astype(BF16)
    return high, (x - high.astype(F32)).astype(BF16)


def as_left(x):
    return jnp.concatenate(halves(x), axis=1)


def as_right(x):
    wide = jnp.concatenate(halves(x), axis=1)
    return jnp.concatenate([wide, wide], axis=0)


def mm(left, right):
    both = jnp.dot(left, right, preferred_element_type=F32)
    size = both.shape[1] // 2
    return both[:, :size] + both[:, size:]


def observed_rows(members, selector, values, root):
    ensemble_size = members.shape[0]
    sampled = jnp.dot(members, selector, preferred_element_type=F32)
    obs_mean = jnp.sum(sampled, axis=0, keepdims=True) * (1.0 / ensemble_size)
    upper = ((sampled - obs_mean) * root).astype(BF16)
    lower = root * (values - obs_mean)
    place = lax.broadcasted_iota(jnp.int32, (16, lower.shape[1]), 0)
    lower = jnp.where(place == 0, jnp.broadcast_to(lower, place.shape), 0.0).astype(BF16)
    return jnp.concatenate([upper, lower], axis=0)


def increments_of(localized, members):
    ensemble_size = members.shape[0]
    row = lax.broadcasted_iota(jnp.int32, (ensemble_size, ensemble_size), 0)
    column = lax.broadcasted_iota(jnp.int32, (ensemble_size, ensemble_size), 1)
    identity = (row == column).astype(F32)
    system = (ensemble_size - 1) / inflation * identity + localized[:ensemble_size]
    bound_norm = jnp.max(
        jnp.sum(jnp.abs(system), axis=0, keepdims=True), axis=1, keepdims=True
    )
    approx_y = system / bound_norm
    update = 1.5 * identity - 0.5 * approx_y
    approx_z = update
    for iteration in range(1, NS_ITERS):
        approx_y = mm(as_left(approx_y), as_right(update))
        left_z = as_left(approx_z)
        update = 1.5 * identity - 0.5 * mm(left_z, as_right(approx_y))
        approx_z = mm(left_z, as_right(update))
    root_inv = approx_z / jnp.sqrt(bound_norm)
    right_r = as_right(root_inv)
    inner = mm(as_left(localized[ensemble_size:]), right_r)
    mean_weights = mm(as_left(inner), right_r)[0:1]
    mixing = jnp.sqrt(F32(ensemble_size - 1)) * root_inv + mean_weights - identity
    high, low = halves(mixing)
    row_sum = jnp.sum(high.astype(F32) + low.astype(F32), axis=1, keepdims=True)
    average = jnp.sum(members.astype(F32), axis=0, keepdims=True) * (1.0 / ensemble_size)
    total = jnp.dot(
        jnp.concatenate([high, low], axis=1),
        jnp.concatenate([members, members], axis=0),
        preferred_element_type=F32,
    )
    return (total - row_sum * average).astype(BF16)


def kernel(
    groups,
    ens_hbm,
    cell,
    count,
    value,
    rinv,
    out,
    arrived,
    rows,
    gram,
    selector,
    stage,
    weight,
    ens,
    load_sem,
    own_sem,
    fwd_send,
    fwd_recv,
    ret_send,
    ret_recv,
    halo_send,
    halo_recv,
):
    me = lax.axis_index("mem")
    blocks, _, width = arrived.shape
    local = ens.shape[0]
    slots = cell.shape[1]
    size = groups * local

    load = pltpu.make_async_copy(ens_hbm, ens, load_sem)
    load.start()
    barrier = pltpu.get_barrier_semaphore()
    for step in range(1, groups):
        pl.semaphore_signal(
            barrier, inc=1, device_id={"mem": lax.rem(me + step, groups)}, device_id_type=MESH
        )

    weight[...] = jnp.sqrt(rinv[...])

    @pl.loop(0, blocks)
    def _(b):
        positions = lax.broadcasted_iota(jnp.int32, (width, slots), 0)
        selector[b] = jnp.where(positions == cell[pl.ds(b, 1), :], 1.0, 0.0).astype(BF16)

    load.wait()
    pl.semaphore_wait(barrier, groups - 1)

    def columns(owner, b):
        start = pl.multiple_of((owner * blocks + b) * width, width)
        return pl.ds(start, width)

    def members_of(owner):
        return pl.ds(pl.multiple_of(owner * local, local), local)

    def send_block(i):
        b = lax.rem(i + blocks - 1, blocks)
        for step in range(1, groups):
            peer = lax.rem(me + step, groups)
            pltpu.make_async_remote_copy(
                src_ref=ens.at[:, columns(peer, b)],
                dst_ref=arrived.at[b, members_of(me), :],
                send_sem=fwd_send,
                recv_sem=fwd_recv.at[b],
                device_id={"mem": peer},
                device_id_type=MESH,
            ).start()
        pltpu.make_async_copy(
            ens.at[:, columns(me, b)], arrived.at[b, members_of(me), :], fwd_recv.at[b]
        ).start()

    for i in range(min(WINDOW, blocks)):
        send_block(i)

    def send_ahead(i):
        @pl.when(i + WINDOW < blocks)
        def _():
            send_block(i + WINDOW)

    def form_gram(slot):
        held = rows[slot]
        gram[slot] = lax.dot_general(
            held, held[:size], (((1,), (1,)), ((), ())), preferred_element_type=F32
        )

    def take_block(b):
        pltpu.make_async_copy(arrived.at[b], arrived.at[b], fwd_recv.at[b]).wait()
        send_ahead(lax.rem(jnp.int32(b) + 1, blocks))
        alive = lax.broadcasted_iota(jnp.int32, (1, slots), 1) < count[0, b]
        root = jnp.where(alive, weight[pl.ds(b, 1), :], 0.0)
        rows[b + 1] = observed_rows(arrived[b], selector[b], value[pl.ds(b, 1), :], root)

    def give_block(b):
        localized = gram[b + 1] + localize * (gram[b] + gram[b + 2])
        stage[b] = increments_of(localized, arrived[b])
        for step in range(1, groups):
            peer = lax.rem(me + step, groups)
            pltpu.make_async_remote_copy(
                src_ref=stage.at[b, members_of(peer), :],
                dst_ref=out.at[:, columns(me, b)],
                send_sem=ret_send,
                recv_sem=ret_recv,
                device_id={"mem": peer},
                device_id_type=MESH,
            ).start()
        pltpu.make_async_copy(
            stage.at[b, members_of(me), :], out.at[:, columns(me, b)], own_sem
        ).start()

    def halo(source, target, peer, which):
        return pltpu.make_async_remote_copy(
            src_ref=rows.at[source],
            dst_ref=rows.at[target],
            send_sem=halo_send.at[which],
            recv_sem=halo_recv.at[which],
            device_id={"mem": peer},
            device_id_type=MESH,
        )

    upward = halo(blocks, 0, lax.rem(me + 1, groups), 0)
    downward = halo(1, blocks + 1, lax.rem(me + groups - 1, groups), 1)

    take_block(blocks - 1)
    upward.start()
    form_gram(blocks)
    take_block(0)
    downward.start()
    form_gram(1)
    take_block(1)
    form_gram(2)
    upward.wait_recv()
    form_gram(0)
    give_block(0)

    @pl.loop(2, blocks - 1)
    def _(b):
        take_block(b)
        form_gram(b + 1)
        give_block(b - 1)

    downward.wait_recv()
    form_gram(blocks + 1)

    @pl.loop(blocks - 2, blocks)
    def _(b):
        give_block(b)

    upward.wait_send()
    downward.wait_send()
    share = blocks * width
    afar = pl.ds(0, (groups - 1) * share)
    pltpu.make_async_copy(ens.at[:, afar], ens.at[:, afar], fwd_send).wait()
    pltpu.make_async_copy(out.at[:, afar], out.at[:, afar], ret_send).wait()
    pltpu.make_async_copy(out.at[:, afar], out.at[:, afar], ret_recv).wait()
    near = pl.ds(0, share)
    pltpu.make_async_copy(out.at[:, near], out.at[:, near], own_sem).wait()


def fused(ensemble, obs_cell, obs_count, obs_value, obs_rinv):
    groups = lax.axis_size("mem")
    local, cells = ensemble.shape
    blocks, slots = obs_cell.shape[1:]
    width = cells // (groups * blocks)
    size = groups * local
    whole = pl.BlockSpec(memory_space=pltpu.VMEM)
    return pl.pallas_call(
        functools.partial(kernel, groups),
        out_shape=jax.ShapeDtypeStruct(ensemble.shape, BF16),
        in_specs=[pl.BlockSpec(memory_space=pl.ANY), whole, pl.BlockSpec(memory_space=pltpu.SMEM), whole, whole],
        out_specs=pl.BlockSpec(memory_space=pl.ANY),
        scratch_shapes=[
            pltpu.VMEM((blocks, size, width), BF16),
            pltpu.VMEM((blocks + 2, size + 16, slots), BF16),
            pltpu.VMEM((blocks + 2, size + 16, size), F32),
            pltpu.VMEM((blocks, width, slots), BF16),
            pltpu.VMEM((blocks, size, width), BF16),
            pltpu.VMEM((blocks, slots), F32),
            pltpu.VMEM(ensemble.shape, BF16),
            pltpu.SemaphoreType.DMA,
            pltpu.SemaphoreType.DMA,
            pltpu.SemaphoreType.DMA,
            pltpu.SemaphoreType.DMA((blocks,)),
            pltpu.SemaphoreType.DMA,
            pltpu.SemaphoreType.DMA,
            pltpu.SemaphoreType.DMA((2,)),
            pltpu.SemaphoreType.DMA((2,)),
        ],
        compiler_params=pltpu.CompilerParams(collective_id=0, has_side_effects=True),
        name="letkf",
    )(ensemble, obs_cell[0], obs_count, obs_value[0], obs_rinv[0])


def with_halo(block, sides, width):
    for axis, dim in sides:
        count = lax.axis_size(axis)
        forward = [(i, i + 1) for i in range(count - 1)]
        forward.append((count - 1, 0))
        backward = [(target, source) for source, target in forward]
        low = lax.ppermute(
            lax.slice_in_dim(block, block.shape[dim] - width, None, axis=dim), axis, forward
        )
        high = lax.ppermute(lax.slice_in_dim(block, 0, width, axis=dim), axis, backward)
        block = jnp.concatenate([low, block, high], axis=dim)
    return block


def center_blocks(members):
    values = jnp.transpose(members.astype(jnp.float32), (1, 0, 2))
    average = jnp.mean(values, axis=1)
    return (values - average[:, None, :], average)


def observe(deviation, average, cell_ids, live_counts, obs_values, inv_var):
    cell_width = deviation.shape[2]
    positions = lax.broadcasted_iota(jnp.int32, cell_ids.shape + (cell_width,), 2)
    selector = (positions == cell_ids[:, :, None]).astype(jnp.float32)
    sampled = jnp.einsum("bkc,boc->bko", deviation, selector, precision=lax.Precision.HIGHEST)
    obs_mean = jnp.einsum("bc,boc->bo", average, selector, precision=lax.Precision.HIGHEST)
    slots = lax.broadcasted_iota(jnp.int32, cell_ids.shape, 1)
    live = (slots < live_counts[:, None]).astype(jnp.float32)
    weight_root = live * jnp.sqrt(inv_var)
    upper = sampled * weight_root[:, None, :]
    lower = (weight_root * (obs_values - obs_mean))[:, None, :]
    return jnp.concatenate([upper, lower], axis=1).astype(jnp.bfloat16)


def gram_of(obs_rows):
    return jnp.einsum("bko,bjo->bkj", obs_rows, obs_rows, preferred_element_type=jnp.float32)


def batch_mm(left, right):
    return jnp.einsum("bij,bjk->bik", left, right, precision=lax.Precision.HIGHEST)


def transform_apply(localized, deviation):
    ensemble_size = deviation.shape[1]
    identity = jnp.eye(ensemble_size, dtype=jnp.float32)
    system = (ensemble_size - 1) / inflation * identity + localized[
        :, :ensemble_size, :ensemble_size
    ]
    forcing = localized[:, :ensemble_size, ensemble_size]
    bound_norm = jnp.max(jnp.sum(jnp.abs(system), axis=2), axis=1)
    approx_y = system / bound_norm[:, None, None]
    approx_z = jnp.broadcast_to(identity, system.shape)
    for iteration in range(NS_ITERS):
        update = 1.5 * identity - 0.5 * batch_mm(approx_z, approx_y)
        approx_y = batch_mm(approx_y, update)
        approx_z = batch_mm(update, approx_z)
    root_inv = approx_z / jnp.sqrt(bound_norm)[:, None, None]
    inner = jnp.einsum("bij,bj->bi", root_inv, forcing, precision=lax.Precision.HIGHEST)
    mean_weights = jnp.einsum("bij,bj->bi", root_inv, inner, precision=lax.Precision.HIGHEST)
    mixing = (
        jnp.sqrt(jnp.float32(ensemble_size - 1)) * root_inv + mean_weights[:, :, None] - identity
    )
    increment = jnp.einsum("bjc,bjk->kbc", deviation, mixing, precision=lax.Precision.HIGHEST)
    return increment.astype(jnp.bfloat16)


def on_device(ensemble, obs_cell, obs_count, obs_value, obs_rinv):
    groups = lax.axis_size("mem")
    local_members = ensemble.shape[0]
    blocks = obs_cell.shape[1]
    cell_width = ensemble.shape[1] // (groups * blocks)
    pieces = ensemble.reshape(local_members, groups, blocks, cell_width)
    arrived = lax.all_to_all(pieces, "mem", split_axis=1, concat_axis=0, tiled=True)
    deviation, average = center_blocks(arrived[:, 0])
    obs_rows = observe(deviation, average, obs_cell[0], obs_count[0], obs_value[0], obs_rinv[0])
    padded_rows = with_halo(obs_rows, (("mem", 0),), 1)
    padded = gram_of(padded_rows)
    localized = padded[1:-1] + localize * (padded[:-2] + padded[2:])
    increment = transform_apply(localized, deviation)
    ensemble_size = increment.shape[0]
    outgoing = increment.reshape(ensemble_size, 1, blocks * cell_width)
    returned = lax.all_to_all(outgoing, "mem", split_axis=0, concat_axis=1, tiled=True)
    return returned.reshape(local_members, groups * blocks * cell_width)


def by_shape(ensemble, *observations):
    groups = lax.axis_size("mem")
    local, cells = ensemble.shape
    blocks, slots = observations[0].shape[1:]
    width = cells // (groups * blocks)
    aligned = local % 16 == 0 and width % 128 == 0 and slots % 128 == 0
    aligned = aligned and (groups * local) % 128 == 0 and groups > 1 and blocks > 2
    return (fused if aligned else on_device)(ensemble, *observations)


def solution(mesh):
    placed = (
        P("mem", "blk"),
        P("blk", "mem", None),
        P("blk", "mem"),
        P("blk", "mem", None),
        P("blk", "mem", None),
    )
    return jax.shard_map(
        by_shape, mesh=mesh, in_specs=placed, out_specs=P("mem", "blk"), check_vma=False
    )
```

```python
import functools

import jax
import jax.numpy as jnp
from jax import lax
from jax.experimental import pallas as pl
from jax.experimental.pallas import tpu as pltpu
from jax.sharding import PartitionSpec as P

NS_ITERS = 4


localize = 0.5
inflation = 1.1

MESH = pl.DeviceIdType.MESH
WINDOW = 3
F32 = jnp.float32
BF16 = jnp.bfloat16


def halves(x):
    high = x.astype(BF16)
    return high, (x - high.astype(F32)).astype(BF16)


def as_left(x):
    return jnp.concatenate(halves(x), axis=1)


def as_right(x):
    wide = jnp.concatenate(halves(x), axis=1)
    return jnp.concatenate([wide, wide], axis=0)


def mm(left, right):
    both = jnp.dot(left, right, preferred_element_type=F32)
    size = both.shape[1] // 2
    return both[:, :size] + both[:, size:]


def observed_rows(members, selector, values, root):
    ensemble_size = members.shape[0]
    sampled = jnp.dot(members, selector, preferred_element_type=F32)
    obs_mean = jnp.sum(sampled, axis=0, keepdims=True) * (1.0 / ensemble_size)
    upper = ((sampled - obs_mean) * root).astype(BF16)
    lower = root * (values - obs_mean)
    place = lax.broadcasted_iota(jnp.int32, (16, lower.shape[1]), 0)
    lower = jnp.where(place == 0, jnp.broadcast_to(lower, place.shape), 0.0).astype(BF16)
    return jnp.concatenate([upper, lower], axis=0)


def increments_of(localized, members):
    ensemble_size = members.shape[0]
    row = lax.broadcasted_iota(jnp.int32, (ensemble_size, ensemble_size), 0)
    column = lax.broadcasted_iota(jnp.int32, (ensemble_size, ensemble_size), 1)
    identity = (row == column).astype(F32)
    system = (ensemble_size - 1) / inflation * identity + localized[:ensemble_size]
    bound_norm = jnp.max(
        jnp.sum(jnp.abs(system), axis=0, keepdims=True), axis=1, keepdims=True
    )
    approx_y = system / bound_norm
    update = 1.5 * identity - 0.5 * approx_y
    approx_z = update
    for iteration in range(1, NS_ITERS):
        approx_y = mm(as_left(approx_y), as_right(update))
        left_z = as_left(approx_z)
        update = 1.5 * identity - 0.5 * mm(left_z, as_right(approx_y))
        approx_z = mm(left_z, as_right(update))
    root_inv = approx_z / jnp.sqrt(bound_norm)
    right_r = as_right(root_inv)
    inner = mm(as_left(localized[ensemble_size:]), right_r)
    mean_weights = mm(as_left(inner), right_r)[0:1]
    mixing = jnp.sqrt(F32(ensemble_size - 1)) * root_inv + mean_weights - identity
    high, low = halves(mixing)
    row_sum = jnp.sum(high.astype(F32) + low.astype(F32), axis=1, keepdims=True)
    average = jnp.sum(members.astype(F32), axis=0, keepdims=True) * (1.0 / ensemble_size)
    total = jnp.dot(
        jnp.concatenate([high, low], axis=1),
        jnp.concatenate([members, members], axis=0),
        preferred_element_type=F32,
    )
    return (total - row_sum * average).astype(BF16)


def kernel(
    groups,
    ens_hbm,
    cell_hbm,
    count_hbm,
    value_hbm,
    rinv_hbm,
    out,
    arrived,
    rows,
    gram,
    selector,
    stage,
    weight,
    ens,
    cell,
    count,
    value,
    rinv,
    load_sem,
    own_sem,
    fwd_send,
    fwd_recv,
    ret_send,
    ret_recv,
    halo_send,
    halo_recv,
):
    me = lax.axis_index("mem")
    blocks, _, width = arrived.shape
    local = ens.shape[0]
    slots = cell.shape[1]
    size = groups * local

    barrier = pltpu.get_barrier_semaphore()
    for step in range(1, groups):
        pl.semaphore_signal(
            barrier, inc=1, device_id={"mem": lax.rem(me + step, groups)}, device_id_type=MESH
        )

    loads = [
        pltpu.make_async_copy(source, target, load_sem.at[i])
        for i, (source, target) in enumerate(
            (
                (ens_hbm, ens),
                (cell_hbm, cell),
                (count_hbm, count),
                (value_hbm, value),
                (rinv_hbm, rinv),
            )
        )
    ]
    for load in loads:
        load.start()
    loads[0].wait()
    pl.semaphore_wait(barrier, groups - 1)

    def columns(owner, b):
        start = pl.multiple_of((owner * blocks + b) * width, width)
        return pl.ds(start, width)

    def members_of(owner):
        return pl.ds(pl.multiple_of(owner * local, local), local)

    def send_block(i):
        b = lax.rem(i + blocks - 1, blocks)
        for step in range(1, groups):
            peer = lax.rem(me + step, groups)
            pltpu.make_async_remote_copy(
                src_ref=ens.at[:, columns(peer, b)],
                dst_ref=arrived.at[b, members_of(me), :],
                send_sem=fwd_send,
                recv_sem=fwd_recv.at[b],
                device_id={"mem": peer},
                device_id_type=MESH,
            ).start()
        pltpu.make_async_copy(
            ens.at[:, columns(me, b)], arrived.at[b, members_of(me), :], fwd_recv.at[b]
        ).start()

    for i in range(min(WINDOW, blocks)):
        send_block(i)

    def send_ahead(i):
        @pl.when(i + WINDOW < blocks)
        def _():
            send_block(i + WINDOW)

    for load in loads[1:]:
        load.wait()
    weight[...] = jnp.sqrt(rinv[...])

    @pl.loop(0, blocks)
    def _(b):
        positions = lax.broadcasted_iota(jnp.int32, (width, slots), 0)
        selector[b] = jnp.where(positions == cell[pl.ds(b, 1), :], 1.0, 0.0).astype(BF16)

    def form_gram(slot):
        held = rows[slot]
        gram[slot] = lax.dot_general(
            held, held[:size], (((1,), (1,)), ((), ())), preferred_element_type=F32
        )

    def take_block(b):
        pltpu.make_async_copy(arrived.at[b], arrived.at[b], fwd_recv.at[b]).wait()
        send_ahead(lax.rem(jnp.int32(b) + 1, blocks))
        alive = lax.broadcasted_iota(jnp.int32, (1, slots), 1) < count[0, b]
        root = jnp.where(alive, weight[pl.ds(b, 1), :], 0.0)
        rows[b + 1] = observed_rows(arrived[b], selector[b], value[pl.ds(b, 1), :], root)

    def give_block(b):
        localized = gram[b + 1] + localize * (gram[b] + gram[b + 2])
        stage[b] = increments_of(localized, arrived[b])
        for step in range(1, groups):
            peer = lax.rem(me + step, groups)
            pltpu.make_async_remote_copy(
                src_ref=stage.at[b, members_of(peer), :],
                dst_ref=out.at[:, columns(me, b)],
                send_sem=ret_send,
                recv_sem=ret_recv,
                device_id={"mem": peer},
                device_id_type=MESH,
            ).start()
        pltpu.make_async_copy(
            stage.at[b, members_of(me), :], out.at[:, columns(me, b)], own_sem
        ).start()

    def halo(source, target, peer, which):
        return pltpu.make_async_remote_copy(
            src_ref=rows.at[source],
            dst_ref=rows.at[target],
            send_sem=halo_send.at[which],
            recv_sem=halo_recv.at[which],
            device_id={"mem": peer},
            device_id_type=MESH,
        )

    upward = halo(blocks, 0, lax.rem(me + 1, groups), 0)
    downward = halo(1, blocks + 1, lax.rem(me + groups - 1, groups), 1)

    take_block(blocks - 1)
    upward.start()
    form_gram(blocks)
    take_block(0)
    downward.start()
    form_gram(1)
    take_block(1)
    form_gram(2)
    upward.wait_recv()
    form_gram(0)
    give_block(0)

    @pl.loop(2, blocks - 1)
    def _(b):
        take_block(b)
        form_gram(b + 1)
        give_block(b - 1)

    downward.wait_recv()
    form_gram(blocks + 1)

    @pl.loop(blocks - 2, blocks)
    def _(b):
        give_block(b)

    upward.wait_send()
    downward.wait_send()
    share = blocks * width
    afar = pl.ds(0, (groups - 1) * share)
    pltpu.make_async_copy(ens.at[:, afar], ens.at[:, afar], fwd_send).wait()
    pltpu.make_async_copy(out.at[:, afar], out.at[:, afar], ret_send).wait()
    pltpu.make_async_copy(out.at[:, afar], out.at[:, afar], ret_recv).wait()
    near = pl.ds(0, share)
    pltpu.make_async_copy(out.at[:, near], out.at[:, near], own_sem).wait()


def fused(ensemble, obs_cell, obs_count, obs_value, obs_rinv):
    groups = lax.axis_size("mem")
    local, cells = ensemble.shape
    blocks, slots = obs_cell.shape[1:]
    width = cells // (groups * blocks)
    size = groups * local
    whole = pl.BlockSpec(memory_space=pltpu.VMEM)
    return pl.pallas_call(
        functools.partial(kernel, groups),
        out_shape=pltpu.VMEM(ensemble.shape, BF16),
        in_specs=[pl.BlockSpec(memory_space=pl.ANY)] * 5,
        out_specs=whole,
        scratch_shapes=[
            pltpu.VMEM((blocks, size, width), BF16),
            pltpu.VMEM((blocks + 2, size + 16, slots), BF16),
            pltpu.VMEM((blocks + 2, size + 16, size), F32),
            pltpu.VMEM((blocks, width, slots), BF16),
            pltpu.VMEM((blocks, size, width), BF16),
            pltpu.VMEM((blocks, slots), F32),
            pltpu.VMEM(ensemble.shape, BF16),
            pltpu.VMEM((blocks, slots), jnp.int32),
            pltpu.SMEM(obs_count.shape, jnp.int32),
            pltpu.VMEM((blocks, slots), F32),
            pltpu.VMEM((blocks, slots), F32),
            pltpu.SemaphoreType.DMA((5,)),
            pltpu.SemaphoreType.DMA,
            pltpu.SemaphoreType.DMA,
            pltpu.SemaphoreType.DMA((blocks,)),
            pltpu.SemaphoreType.DMA,
            pltpu.SemaphoreType.DMA,
            pltpu.SemaphoreType.DMA((2,)),
            pltpu.SemaphoreType.DMA((2,)),
        ],
        compiler_params=pltpu.CompilerParams(collective_id=0, has_side_effects=True),
        name="letkf",
    )(ensemble, obs_cell[0], obs_count, obs_value[0], obs_rinv[0])


def with_halo(block, sides, width):
    for axis, dim in sides:
        count = lax.axis_size(axis)
        forward = [(i, i + 1) for i in range(count - 1)]
        forward.append((count - 1, 0))
        backward = [(target, source) for source, target in forward]
        low = lax.ppermute(
            lax.slice_in_dim(block, block.shape[dim] - width, None, axis=dim), axis, forward
        )
        high = lax.ppermute(lax.slice_in_dim(block, 0, width, axis=dim), axis, backward)
        block = jnp.concatenate([low, block, high], axis=dim)
    return block


def center_blocks(members):
    values = jnp.transpose(members.astype(jnp.float32), (1, 0, 2))
    average = jnp.mean(values, axis=1)
    return (values - average[:, None, :], average)


def observe(deviation, average, cell_ids, live_counts, obs_values, inv_var):
    cell_width = deviation.shape[2]
    positions = lax.broadcasted_iota(jnp.int32, cell_ids.shape + (cell_width,), 2)
    selector = (positions == cell_ids[:, :, None]).astype(jnp.float32)
    sampled = jnp.einsum("bkc,boc->bko", deviation, selector, precision=lax.Precision.HIGHEST)
    obs_mean = jnp.einsum("bc,boc->bo", average, selector, precision=lax.Precision.HIGHEST)
    slots = lax.broadcasted_iota(jnp.int32, cell_ids.shape, 1)
    live = (slots < live_counts[:, None]).astype(jnp.float32)
    weight_root = live * jnp.sqrt(inv_var)
    upper = sampled * weight_root[:, None, :]
    lower = (weight_root * (obs_values - obs_mean))[:, None, :]
    return jnp.concatenate([upper, lower], axis=1).astype(jnp.bfloat16)


def gram_of(obs_rows):
    return jnp.einsum("bko,bjo->bkj", obs_rows, obs_rows, preferred_element_type=jnp.float32)


def batch_mm(left, right):
    return jnp.einsum("bij,bjk->bik", left, right, precision=lax.Precision.HIGHEST)


def transform_apply(localized, deviation):
    ensemble_size = deviation.shape[1]
    identity = jnp.eye(ensemble_size, dtype=jnp.float32)
    system = (ensemble_size - 1) / inflation * identity + localized[
        :, :ensemble_size, :ensemble_size
    ]
    forcing = localized[:, :ensemble_size, ensemble_size]
    bound_norm = jnp.max(jnp.sum(jnp.abs(system), axis=2), axis=1)
    approx_y = system / bound_norm[:, None, None]
    approx_z = jnp.broadcast_to(identity, system.shape)
    for iteration in range(NS_ITERS):
        update = 1.5 * identity - 0.5 * batch_mm(approx_z, approx_y)
        approx_y = batch_mm(approx_y, update)
        approx_z = batch_mm(update, approx_z)
    root_inv = approx_z / jnp.sqrt(bound_norm)[:, None, None]
    inner = jnp.einsum("bij,bj->bi", root_inv, forcing, precision=lax.Precision.HIGHEST)
    mean_weights = jnp.einsum("bij,bj->bi", root_inv, inner, precision=lax.Precision.HIGHEST)
    mixing = (
        jnp.sqrt(jnp.float32(ensemble_size - 1)) * root_inv + mean_weights[:, :, None] - identity
    )
    increment = jnp.einsum("bjc,bjk->kbc", deviation, mixing, precision=lax.Precision.HIGHEST)
    return increment.astype(jnp.bfloat16)


def on_device(ensemble, obs_cell, obs_count, obs_value, obs_rinv):
    groups = lax.axis_size("mem")
    local_members = ensemble.shape[0]
    blocks = obs_cell.shape[1]
    cell_width = ensemble.shape[1] // (groups * blocks)
    pieces = ensemble.reshape(local_members, groups, blocks, cell_width)
    arrived = lax.all_to_all(pieces, "mem", split_axis=1, concat_axis=0, tiled=True)
    deviation, average = center_blocks(arrived[:, 0])
    obs_rows = observe(deviation, average, obs_cell[0], obs_count[0], obs_value[0], obs_rinv[0])
    padded_rows = with_halo(obs_rows, (("mem", 0),), 1)
    padded = gram_of(padded_rows)
    localized = padded[1:-1] + localize * (padded[:-2] + padded[2:])
    increment = transform_apply(localized, deviation)
    ensemble_size = increment.shape[0]
    outgoing = increment.reshape(ensemble_size, 1, blocks * cell_width)
    returned = lax.all_to_all(outgoing, "mem", split_axis=0, concat_axis=1, tiled=True)
    return returned.reshape(local_members, groups * blocks * cell_width)


def by_shape(ensemble, *observations):
    groups = lax.axis_size("mem")
    local, cells = ensemble.shape
    blocks, slots = observations[0].shape[1:]
    width = cells // (groups * blocks)
    aligned = local % 16 == 0 and width % 128 == 0 and slots % 128 == 0
    aligned = aligned and (groups * local) % 128 == 0 and groups > 1 and blocks > 2
    return (fused if aligned else on_device)(ensemble, *observations)


def solution(mesh):
    placed = (
        P("mem", "blk"),
        P("blk", "mem", None),
        P("blk", "mem"),
        P("blk", "mem", None),
        P("blk", "mem", None),
    )
    return jax.shard_map(
        by_shape, mesh=mesh, in_specs=placed, out_specs=P("mem", "blk"), check_vma=False
    )
```

```python
import functools

import jax
import jax.numpy as jnp
from jax import lax
from jax.experimental import pallas as pl
from jax.experimental.pallas import tpu as pltpu
from jax.sharding import PartitionSpec as P

NS_ITERS = 4


localize = 0.5
inflation = 1.1

MESH = pl.DeviceIdType.MESH
WINDOW = 3
F32 = jnp.float32
BF16 = jnp.bfloat16


def halves(x):
    high = x.astype(BF16)
    return high, (x - high.astype(F32)).astype(BF16)


def as_left(x):
    return jnp.concatenate(halves(x), axis=1)


def as_right(x):
    wide = jnp.concatenate(halves(x), axis=1)
    return jnp.concatenate([wide, wide], axis=0)


def mm(left, right):
    both = jnp.dot(left, right, preferred_element_type=F32)
    size = both.shape[1] // 2
    return both[:, :size] + both[:, size:]


def observed_rows(members, selector, values, root):
    ensemble_size = members.shape[0]
    sampled = jnp.dot(members, selector, preferred_element_type=F32)
    obs_mean = jnp.sum(sampled, axis=0, keepdims=True) * (1.0 / ensemble_size)
    upper = ((sampled - obs_mean) * root).astype(BF16)
    lower = root * (values - obs_mean)
    place = lax.broadcasted_iota(jnp.int32, (16, lower.shape[1]), 0)
    lower = jnp.where(place == 0, jnp.broadcast_to(lower, place.shape), 0.0).astype(BF16)
    return jnp.concatenate([upper, lower], axis=0)


def increments_of(localized, members):
    ensemble_size = members.shape[0]
    row = lax.broadcasted_iota(jnp.int32, (ensemble_size, ensemble_size), 0)
    column = lax.broadcasted_iota(jnp.int32, (ensemble_size, ensemble_size), 1)
    identity = (row == column).astype(F32)
    system = (ensemble_size - 1) / inflation * identity + localized[:ensemble_size]
    bound_norm = jnp.max(
        jnp.sum(jnp.abs(system), axis=0, keepdims=True), axis=1, keepdims=True
    )
    approx_y = system / bound_norm
    update = 1.5 * identity - 0.5 * approx_y
    approx_z = update
    for iteration in range(1, NS_ITERS):
        approx_y = mm(as_left(approx_y), as_right(update))
        left_z = as_left(approx_z)
        update = 1.5 * identity - 0.5 * mm(left_z, as_right(approx_y))
        approx_z = mm(left_z, as_right(update))
    root_inv = approx_z / jnp.sqrt(bound_norm)
    right_r = as_right(root_inv)
    inner = mm(as_left(localized[ensemble_size:]), right_r)
    mean_weights = mm(as_left(inner), right_r)[0:1]
    mixing = jnp.sqrt(F32(ensemble_size - 1)) * root_inv + mean_weights - identity
    high, low = halves(mixing)
    row_sum = jnp.sum(high.astype(F32) + low.astype(F32), axis=1, keepdims=True)
    average = jnp.sum(members.astype(F32), axis=0, keepdims=True) * (1.0 / ensemble_size)
    total = jnp.dot(
        jnp.concatenate([high, low], axis=1),
        jnp.concatenate([members, members], axis=0),
        preferred_element_type=F32,
    )
    return (total - row_sum * average).astype(BF16)


def kernel(
    groups,
    ens_hbm,
    cell_hbm,
    count_hbm,
    value_hbm,
    rinv_hbm,
    out,
    arrived,
    rows,
    gram,
    edge,
    far_edge,
    selector,
    stage,
    weight,
    ens,
    cell,
    count,
    value,
    rinv,
    load_sem,
    own_sem,
    fwd_send,
    fwd_recv,
    ret_send,
    ret_recv,
    halo_send,
    halo_recv,
):
    me = lax.axis_index("mem")
    blocks, _, width = arrived.shape
    local = ens.shape[0]
    slots = cell.shape[1]
    size = groups * local

    barrier = pltpu.get_barrier_semaphore()
    for step in range(1, groups):
        pl.semaphore_signal(
            barrier, inc=1, device_id={"mem": lax.rem(me + step, groups)}, device_id_type=MESH
        )

    loads = [
        pltpu.make_async_copy(source, target, load_sem.at[i])
        for i, (source, target) in enumerate(
            (
                (ens_hbm, ens),
                (cell_hbm, cell),
                (count_hbm, count),
                (value_hbm, value),
                (rinv_hbm, rinv),
            )
        )
    ]
    for load in loads:
        load.start()
    loads[0].wait()
    pl.semaphore_wait(barrier, groups - 1)

    def columns(owner, b):
        start = pl.multiple_of((owner * blocks + b) * width, width)
        return pl.ds(start, width)

    def members_of(owner):
        return pl.ds(pl.multiple_of(owner * local, local), local)

    def send_block(i):
        b = lax.rem(i + blocks - 1, blocks)
        for step in range(1, groups):
            peer = lax.rem(me + step, groups)
            pltpu.make_async_remote_copy(
                src_ref=ens.at[:, columns(peer, b)],
                dst_ref=arrived.at[b, members_of(me), :],
                send_sem=fwd_send,
                recv_sem=fwd_recv.at[b],
                device_id={"mem": peer},
                device_id_type=MESH,
            ).start()
        pltpu.make_async_copy(
            ens.at[:, columns(me, b)], arrived.at[b, members_of(me), :], fwd_recv.at[b]
        ).start()

    for i in range(min(WINDOW, blocks)):
        send_block(i)

    def send_ahead(i):
        @pl.when(i + WINDOW < blocks)
        def _():
            send_block(i + WINDOW)

    for load in loads[1:]:
        load.wait()
    weight[...] = jnp.sqrt(rinv[...])

    @pl.loop(0, blocks)
    def _(b):
        positions = lax.broadcasted_iota(jnp.int32, (width, slots), 0)
        selector[b] = jnp.where(positions == cell[pl.ds(b, 1), :], 1.0, 0.0).astype(BF16)

    def form_gram(slot):
        held = rows[slot]
        gram[slot] = lax.dot_general(
            held, held[:size], (((1,), (1,)), ((), ())), preferred_element_type=F32
        )

    def take_block(b):
        pltpu.make_async_copy(arrived.at[b], arrived.at[b], fwd_recv.at[b]).wait()
        send_ahead(lax.rem(jnp.int32(b) + 1, blocks))
        alive = lax.broadcasted_iota(jnp.int32, (1, slots), 1) < count[0, b]
        root = jnp.where(alive, weight[pl.ds(b, 1), :], 0.0)
        rows[b + 1] = observed_rows(arrived[b], selector[b], value[pl.ds(b, 1), :], root)

    def give_block(b):
        localized = gram[b + 1] + localize * (gram[b] + gram[b + 2])
        stage[b] = increments_of(localized, arrived[b])
        for step in range(1, groups):
            peer = lax.rem(me + step, groups)
            pltpu.make_async_remote_copy(
                src_ref=stage.at[b, members_of(peer), :],
                dst_ref=out.at[:, columns(me, b)],
                send_sem=ret_send,
                recv_sem=ret_recv,
                device_id={"mem": peer},
                device_id_type=MESH,
            ).start()
        pltpu.make_async_copy(
            stage.at[b, members_of(me), :], out.at[:, columns(me, b)], own_sem
        ).start()

    def halo(slot, peer, which):
        edge[which] = gram[slot].astype(BF16)
        return pltpu.make_async_remote_copy(
            src_ref=edge.at[which],
            dst_ref=far_edge.at[which],
            send_sem=halo_send.at[which],
            recv_sem=halo_recv.at[which],
            device_id={"mem": peer},
            device_id_type=MESH,
        )

    take_block(blocks - 1)
    form_gram(blocks)
    upward = halo(blocks, lax.rem(me + 1, groups), 0)
    upward.start()
    take_block(0)
    form_gram(1)
    downward = halo(1, lax.rem(me + groups - 1, groups), 1)
    downward.start()
    take_block(1)
    form_gram(2)
    upward.wait_recv()
    gram[0] = far_edge[0].astype(F32)
    give_block(0)

    @pl.loop(2, blocks - 1)
    def _(b):
        take_block(b)
        form_gram(b + 1)
        give_block(b - 1)

    downward.wait_recv()
    gram[blocks + 1] = far_edge[1].astype(F32)

    @pl.loop(blocks - 2, blocks)
    def _(b):
        give_block(b)

    upward.wait_send()
    downward.wait_send()
    share = blocks * width
    afar = pl.ds(0, (groups - 1) * share)
    pltpu.make_async_copy(ens.at[:, afar], ens.at[:, afar], fwd_send).wait()
    pltpu.make_async_copy(out.at[:, afar], out.at[:, afar], ret_send).wait()
    pltpu.make_async_copy(out.at[:, afar], out.at[:, afar], ret_recv).wait()
    near = pl.ds(0, share)
    pltpu.make_async_copy(out.at[:, near], out.at[:, near], own_sem).wait()


def fused(ensemble, obs_cell, obs_count, obs_value, obs_rinv):
    groups = lax.axis_size("mem")
    local, cells = ensemble.shape
    blocks, slots = obs_cell.shape[1:]
    width = cells // (groups * blocks)
    size = groups * local
    whole = pl.BlockSpec(memory_space=pltpu.VMEM)
    return pl.pallas_call(
        functools.partial(kernel, groups),
        out_shape=pltpu.VMEM(ensemble.shape, BF16),
        in_specs=[pl.BlockSpec(memory_space=pl.ANY)] * 5,
        out_specs=whole,
        scratch_shapes=[
            pltpu.VMEM((blocks, size, width), BF16),
            pltpu.VMEM((blocks + 2, size + 16, slots), BF16),
            pltpu.VMEM((blocks + 2, size + 16, size), F32),
            pltpu.VMEM((2, size + 16, size), BF16),
            pltpu.VMEM((2, size + 16, size), BF16),
            pltpu.VMEM((blocks, width, slots), BF16),
            pltpu.VMEM((blocks, size, width), BF16),
            pltpu.VMEM((blocks, slots), F32),
            pltpu.VMEM(ensemble.shape, BF16),
            pltpu.VMEM((blocks, slots), jnp.int32),
            pltpu.SMEM(obs_count.shape, jnp.int32),
            pltpu.VMEM((blocks, slots), F32),
            pltpu.VMEM((blocks, slots), F32),
            pltpu.SemaphoreType.DMA((5,)),
            pltpu.SemaphoreType.DMA,
            pltpu.SemaphoreType.DMA,
            pltpu.SemaphoreType.DMA((blocks,)),
            pltpu.SemaphoreType.DMA,
            pltpu.SemaphoreType.DMA,
            pltpu.SemaphoreType.DMA((2,)),
            pltpu.SemaphoreType.DMA((2,)),
        ],
        compiler_params=pltpu.CompilerParams(collective_id=0, has_side_effects=True),
        name="letkf",
    )(ensemble, obs_cell[0], obs_count, obs_value[0], obs_rinv[0])


def with_halo(block, sides, width):
    for axis, dim in sides:
        count = lax.axis_size(axis)
        forward = [(i, i + 1) for i in range(count - 1)]
        forward.append((count - 1, 0))
        backward = [(target, source) for source, target in forward]
        low = lax.ppermute(
            lax.slice_in_dim(block, block.shape[dim] - width, None, axis=dim), axis, forward
        )
        high = lax.ppermute(lax.slice_in_dim(block, 0, width, axis=dim), axis, backward)
        block = jnp.concatenate([low, block, high], axis=dim)
    return block


def center_blocks(members):
    values = jnp.transpose(members.astype(jnp.float32), (1, 0, 2))
    average = jnp.mean(values, axis=1)
    return (values - average[:, None, :], average)


def observe(deviation, average, cell_ids, live_counts, obs_values, inv_var):
    cell_width = deviation.shape[2]
    positions = lax.broadcasted_iota(jnp.int32, cell_ids.shape + (cell_width,), 2)
    selector = (positions == cell_ids[:, :, None]).astype(jnp.float32)
    sampled = jnp.einsum("bkc,boc->bko", deviation, selector, precision=lax.Precision.HIGHEST)
    obs_mean = jnp.einsum("bc,boc->bo", average, selector, precision=lax.Precision.HIGHEST)
    slots = lax.broadcasted_iota(jnp.int32, cell_ids.shape, 1)
    live = (slots < live_counts[:, None]).astype(jnp.float32)
    weight_root = live * jnp.sqrt(inv_var)
    upper = sampled * weight_root[:, None, :]
    lower = (weight_root * (obs_values - obs_mean))[:, None, :]
    return jnp.concatenate([upper, lower], axis=1).astype(jnp.bfloat16)


def gram_of(obs_rows):
    return jnp.einsum("bko,bjo->bkj", obs_rows, obs_rows, preferred_element_type=jnp.float32)


def batch_mm(left, right):
    return jnp.einsum("bij,bjk->bik", left, right, precision=lax.Precision.HIGHEST)


def transform_apply(localized, deviation):
    ensemble_size = deviation.shape[1]
    identity = jnp.eye(ensemble_size, dtype=jnp.float32)
    system = (ensemble_size - 1) / inflation * identity + localized[
        :, :ensemble_size, :ensemble_size
    ]
    forcing = localized[:, :ensemble_size, ensemble_size]
    bound_norm = jnp.max(jnp.sum(jnp.abs(system), axis=2), axis=1)
    approx_y = system / bound_norm[:, None, None]
    approx_z = jnp.broadcast_to(identity, system.shape)
    for iteration in range(NS_ITERS):
        update = 1.5 * identity - 0.5 * batch_mm(approx_z, approx_y)
        approx_y = batch_mm(approx_y, update)
        approx_z = batch_mm(update, approx_z)
    root_inv = approx_z / jnp.sqrt(bound_norm)[:, None, None]
    inner = jnp.einsum("bij,bj->bi", root_inv, forcing, precision=lax.Precision.HIGHEST)
    mean_weights = jnp.einsum("bij,bj->bi", root_inv, inner, precision=lax.Precision.HIGHEST)
    mixing = (
        jnp.sqrt(jnp.float32(ensemble_size - 1)) * root_inv + mean_weights[:, :, None] - identity
    )
    increment = jnp.einsum("bjc,bjk->kbc", deviation, mixing, precision=lax.Precision.HIGHEST)
    return increment.astype(jnp.bfloat16)


def on_device(ensemble, obs_cell, obs_count, obs_value, obs_rinv):
    groups = lax.axis_size("mem")
    local_members = ensemble.shape[0]
    blocks = obs_cell.shape[1]
    cell_width = ensemble.shape[1] // (groups * blocks)
    pieces = ensemble.reshape(local_members, groups, blocks, cell_width)
    arrived = lax.all_to_all(pieces, "mem", split_axis=1, concat_axis=0, tiled=True)
    deviation, average = center_blocks(arrived[:, 0])
    obs_rows = observe(deviation, average, obs_cell[0], obs_count[0], obs_value[0], obs_rinv[0])
    padded_rows = with_halo(obs_rows, (("mem", 0),), 1)
    padded = gram_of(padded_rows)
    localized = padded[1:-1] + localize * (padded[:-2] + padded[2:])
    increment = transform_apply(localized, deviation)
    ensemble_size = increment.shape[0]
    outgoing = increment.reshape(ensemble_size, 1, blocks * cell_width)
    returned = lax.all_to_all(outgoing, "mem", split_axis=0, concat_axis=1, tiled=True)
    return returned.reshape(local_members, groups * blocks * cell_width)


def by_shape(ensemble, *observations):
    groups = lax.axis_size("mem")
    local, cells = ensemble.shape
    blocks, slots = observations[0].shape[1:]
    width = cells // (groups * blocks)
    aligned = local % 16 == 0 and width % 128 == 0 and slots % 128 == 0
    aligned = aligned and (groups * local) % 128 == 0 and groups > 1 and blocks > 2
    return (fused if aligned else on_device)(ensemble, *observations)


def solution(mesh):
    placed = (
        P("mem", "blk"),
        P("blk", "mem", None),
        P("blk", "mem"),
        P("blk", "mem", None),
        P("blk", "mem", None),
    )
    return jax.shard_map(
        by_shape, mesh=mesh, in_specs=placed, out_specs=P("mem", "blk"), check_vma=False
    )
```

```python
import functools

import jax
import jax.numpy as jnp
from jax import lax
from jax.experimental import pallas as pl
from jax.experimental.pallas import tpu as pltpu
from jax.sharding import PartitionSpec as P

NS_ITERS = 4


localize = 0.5
inflation = 1.1

MESH = pl.DeviceIdType.MESH
WINDOW = 3
F32 = jnp.float32
BF16 = jnp.bfloat16


def halves(x):
    high = x.astype(BF16)
    return high, (x - high.astype(F32)).astype(BF16)


def as_left(x):
    return jnp.concatenate(halves(x), axis=1)


def as_right(x):
    wide = jnp.concatenate(halves(x), axis=1)
    return jnp.concatenate([wide, wide], axis=0)


def mm(left, right):
    both = jnp.dot(left, right, preferred_element_type=F32)
    size = both.shape[1] // 2
    return both[:, :size] + both[:, size:]


def observed_rows(members, selector, values, root):
    ensemble_size = members.shape[0]
    sampled = jnp.dot(members, selector, preferred_element_type=F32)
    obs_mean = jnp.sum(sampled, axis=0, keepdims=True) * (1.0 / ensemble_size)
    upper = ((sampled - obs_mean) * root).astype(BF16)
    lower = root * (values - obs_mean)
    place = lax.broadcasted_iota(jnp.int32, (16, lower.shape[1]), 0)
    lower = jnp.where(place == 0, jnp.broadcast_to(lower, place.shape), 0.0).astype(BF16)
    return jnp.concatenate([upper, lower], axis=0)


def increments_of(localized, members):
    ensemble_size = members.shape[0]
    row = lax.broadcasted_iota(jnp.int32, (ensemble_size, ensemble_size), 0)
    column = lax.broadcasted_iota(jnp.int32, (ensemble_size, ensemble_size), 1)
    identity = (row == column).astype(F32)
    system = (ensemble_size - 1) / inflation * identity + localized[:ensemble_size]
    bound_norm = jnp.max(
        jnp.sum(jnp.abs(system), axis=0, keepdims=True), axis=1, keepdims=True
    )
    approx_y = system / bound_norm
    update = 1.5 * identity - 0.5 * approx_y
    approx_z = update
    for iteration in range(1, NS_ITERS):
        approx_y = mm(as_left(approx_y), as_right(update))
        left_z = as_left(approx_z)
        update = 1.5 * identity - 0.5 * mm(left_z, as_right(approx_y))
        approx_z = mm(left_z, as_right(update))
    root_inv = approx_z / jnp.sqrt(bound_norm)
    right_r = as_right(root_inv)
    inner = mm(as_left(localized[ensemble_size:]), right_r)
    mean_weights = mm(as_left(inner), right_r)[0:1]
    mixing = jnp.sqrt(F32(ensemble_size - 1)) * root_inv + mean_weights - identity
    high, low = halves(mixing)
    row_sum = jnp.sum(high.astype(F32) + low.astype(F32), axis=1, keepdims=True)
    average = jnp.sum(members.astype(F32), axis=0, keepdims=True) * (1.0 / ensemble_size)
    total = jnp.dot(
        jnp.concatenate([high, low], axis=1),
        jnp.concatenate([members, members], axis=0),
        preferred_element_type=F32,
    )
    return (total - row_sum * average).astype(BF16)


def kernel(
    groups,
    ens_hbm,
    cell_hbm,
    count_hbm,
    value_hbm,
    rinv_hbm,
    out,
    arrived,
    rows,
    gram,
    edge,
    far_edge,
    selector,
    stage,
    weight,
    ens,
    cell,
    count,
    value,
    rinv,
    load_sem,
    own_sem,
    fwd_send,
    fwd_recv,
    ret_send,
    ret_recv,
    halo_send,
    halo_recv,
):
    me = lax.axis_index("mem")
    blocks, _, width = arrived.shape
    local = ens.shape[0]
    slots = cell.shape[1]
    size = groups * local

    barrier = pltpu.get_barrier_semaphore()
    for step in range(1, groups):
        pl.semaphore_signal(
            barrier, inc=1, device_id={"mem": lax.rem(me + step, groups)}, device_id_type=MESH
        )

    loads = [
        pltpu.make_async_copy(source, target, load_sem.at[i])
        for i, (source, target) in enumerate(
            (
                (ens_hbm, ens),
                (cell_hbm, cell),
                (count_hbm, count),
                (value_hbm, value),
                (rinv_hbm, rinv),
            )
        )
    ]
    for load in loads:
        load.start()
    loads[0].wait()
    pl.semaphore_wait(barrier, groups - 1)

    def columns(owner, b):
        start = pl.multiple_of((owner * blocks + b) * width, width)
        return pl.ds(start, width)

    def members_of(owner):
        return pl.ds(pl.multiple_of(owner * local, local), local)

    def send_block(i):
        b = lax.rem(i + blocks - 1, blocks)
        for step in range(1, groups):
            peer = lax.rem(me + step, groups)
            pltpu.make_async_remote_copy(
                src_ref=ens.at[:, columns(peer, b)],
                dst_ref=arrived.at[b, members_of(me), :],
                send_sem=fwd_send,
                recv_sem=fwd_recv.at[b],
                device_id={"mem": peer},
                device_id_type=MESH,
            ).start()
        pltpu.make_async_copy(
            ens.at[:, columns(me, b)], arrived.at[b, members_of(me), :], fwd_recv.at[b]
        ).start()

    for i in range(min(WINDOW, blocks)):
        send_block(i)

    def send_ahead(i):
        @pl.when(i + WINDOW < blocks)
        def _():
            send_block(i + WINDOW)

    for load in loads[1:]:
        load.wait()
    weight[...] = jnp.sqrt(rinv[...])

    @pl.loop(0, blocks)
    def _(b):
        positions = lax.broadcasted_iota(jnp.int32, (width, slots), 0)
        selector[b] = jnp.where(positions == cell[pl.ds(b, 1), :], 1.0, 0.0).astype(BF16)

    def form_gram(slot):
        held = rows[slot]
        gram[slot] = lax.dot_general(
            held, held[:size], (((1,), (1,)), ((), ())), preferred_element_type=F32
        )

    def take_block(b):
        pltpu.make_async_copy(arrived.at[b], arrived.at[b], fwd_recv.at[b]).wait()
        send_ahead(lax.rem(jnp.int32(b) + 1, blocks))
        alive = lax.broadcasted_iota(jnp.int32, (1, slots), 1) < count[0, b]
        root = jnp.where(alive, weight[pl.ds(b, 1), :], 0.0)
        rows[b + 1] = observed_rows(arrived[b], selector[b], value[pl.ds(b, 1), :], root)

    def give_block(b):
        localized = gram[b + 1] + localize * (gram[b] + gram[b + 2])
        pair = b // 2
        part = pl.ds(pl.multiple_of((b % 2) * width, width), width)
        stage[pair, :, part] = increments_of(localized, arrived[b])

        @pl.when(b % 2 == 1)
        def _():
            both = pl.ds(pl.multiple_of((me * blocks + b - 1) * width, width), 2 * width)
            for step in range(1, groups):
                peer = lax.rem(me + step, groups)
                pltpu.make_async_remote_copy(
                    src_ref=stage.at[pair, members_of(peer), :],
                    dst_ref=out.at[:, both],
                    send_sem=ret_send,
                    recv_sem=ret_recv,
                    device_id={"mem": peer},
                    device_id_type=MESH,
                ).start()
            pltpu.make_async_copy(
                stage.at[pair, members_of(me), :], out.at[:, both], own_sem
            ).start()

    def halo(slot, peer, which):
        edge[which] = gram[slot].astype(BF16)
        return pltpu.make_async_remote_copy(
            src_ref=edge.at[which],
            dst_ref=far_edge.at[which],
            send_sem=halo_send.at[which],
            recv_sem=halo_recv.at[which],
            device_id={"mem": peer},
            device_id_type=MESH,
        )

    take_block(blocks - 1)
    form_gram(blocks)
    upward = halo(blocks, lax.rem(me + 1, groups), 0)
    upward.start()
    take_block(0)
    form_gram(1)
    downward = halo(1, lax.rem(me + groups - 1, groups), 1)
    downward.start()
    take_block(1)
    form_gram(2)
    upward.wait_recv()
    gram[0] = far_edge[0].astype(F32)
    give_block(jnp.int32(0))

    @pl.loop(2, blocks - 1)
    def _(b):
        take_block(b)
        form_gram(b + 1)
        give_block(b - 1)

    downward.wait_recv()
    gram[blocks + 1] = far_edge[1].astype(F32)

    @pl.loop(blocks - 2, blocks)
    def _(b):
        give_block(b)

    upward.wait_send()
    downward.wait_send()
    share = blocks * width
    afar = pl.ds(0, (groups - 1) * share)
    pltpu.make_async_copy(ens.at[:, afar], ens.at[:, afar], fwd_send).wait()
    pltpu.make_async_copy(out.at[:, afar], out.at[:, afar], ret_send).wait()
    pltpu.make_async_copy(out.at[:, afar], out.at[:, afar], ret_recv).wait()
    near = pl.ds(0, share)
    pltpu.make_async_copy(out.at[:, near], out.at[:, near], own_sem).wait()


def fused(ensemble, obs_cell, obs_count, obs_value, obs_rinv):
    groups = lax.axis_size("mem")
    local, cells = ensemble.shape
    blocks, slots = obs_cell.shape[1:]
    width = cells // (groups * blocks)
    size = groups * local
    whole = pl.BlockSpec(memory_space=pltpu.VMEM)
    return pl.pallas_call(
        functools.partial(kernel, groups),
        out_shape=pltpu.VMEM(ensemble.shape, BF16),
        in_specs=[pl.BlockSpec(memory_space=pl.ANY)] * 5,
        out_specs=whole,
        scratch_shapes=[
            pltpu.VMEM((blocks, size, width), BF16),
            pltpu.VMEM((blocks + 2, size + 16, slots), BF16),
            pltpu.VMEM((blocks + 2, size + 16, size), F32),
            pltpu.VMEM((2, size + 16, size), BF16),
            pltpu.VMEM((2, size + 16, size), BF16),
            pltpu.VMEM((blocks, width, slots), BF16),
            pltpu.VMEM((blocks // 2, size, 2 * width), BF16),
            pltpu.VMEM((blocks, slots), F32),
            pltpu.VMEM(ensemble.shape, BF16),
            pltpu.VMEM((blocks, slots), jnp.int32),
            pltpu.SMEM(obs_count.shape, jnp.int32),
            pltpu.VMEM((blocks, slots), F32),
            pltpu.VMEM((blocks, slots), F32),
            pltpu.SemaphoreType.DMA((5,)),
            pltpu.SemaphoreType.DMA,
            pltpu.SemaphoreType.DMA,
            pltpu.SemaphoreType.DMA((blocks,)),
            pltpu.SemaphoreType.DMA,
            pltpu.SemaphoreType.DMA,
            pltpu.SemaphoreType.DMA((2,)),
            pltpu.SemaphoreType.DMA((2,)),
        ],
        compiler_params=pltpu.CompilerParams(collective_id=0, has_side_effects=True),
        name="letkf",
    )(ensemble, obs_cell[0], obs_count, obs_value[0], obs_rinv[0])


def with_halo(block, sides, width):
    for axis, dim in sides:
        count = lax.axis_size(axis)
        forward = [(i, i + 1) for i in range(count - 1)]
        forward.append((count - 1, 0))
        backward = [(target, source) for source, target in forward]
        low = lax.ppermute(
            lax.slice_in_dim(block, block.shape[dim] - width, None, axis=dim), axis, forward
        )
        high = lax.ppermute(lax.slice_in_dim(block, 0, width, axis=dim), axis, backward)
        block = jnp.concatenate([low, block, high], axis=dim)
    return block


def center_blocks(members):
    values = jnp.transpose(members.astype(jnp.float32), (1, 0, 2))
    average = jnp.mean(values, axis=1)
    return (values - average[:, None, :], average)


def observe(deviation, average, cell_ids, live_counts, obs_values, inv_var):
    cell_width = deviation.shape[2]
    positions = lax.broadcasted_iota(jnp.int32, cell_ids.shape + (cell_width,), 2)
    selector = (positions == cell_ids[:, :, None]).astype(jnp.float32)
    sampled = jnp.einsum("bkc,boc->bko", deviation, selector, precision=lax.Precision.HIGHEST)
    obs_mean = jnp.einsum("bc,boc->bo", average, selector, precision=lax.Precision.HIGHEST)
    slots = lax.broadcasted_iota(jnp.int32, cell_ids.shape, 1)
    live = (slots < live_counts[:, None]).astype(jnp.float32)
    weight_root = live * jnp.sqrt(inv_var)
    upper = sampled * weight_root[:, None, :]
    lower = (weight_root * (obs_values - obs_mean))[:, None, :]
    return jnp.concatenate([upper, lower], axis=1).astype(jnp.bfloat16)


def gram_of(obs_rows):
    return jnp.einsum("bko,bjo->bkj", obs_rows, obs_rows, preferred_element_type=jnp.float32)


def batch_mm(left, right):
    return jnp.einsum("bij,bjk->bik", left, right, precision=lax.Precision.HIGHEST)


def transform_apply(localized, deviation):
    ensemble_size = deviation.shape[1]
    identity = jnp.eye(ensemble_size, dtype=jnp.float32)
    system = (ensemble_size - 1) / inflation * identity + localized[
        :, :ensemble_size, :ensemble_size
    ]
    forcing = localized[:, :ensemble_size, ensemble_size]
    bound_norm = jnp.max(jnp.sum(jnp.abs(system), axis=2), axis=1)
    approx_y = system / bound_norm[:, None, None]
    approx_z = jnp.broadcast_to(identity, system.shape)
    for iteration in range(NS_ITERS):
        update = 1.5 * identity - 0.5 * batch_mm(approx_z, approx_y)
        approx_y = batch_mm(approx_y, update)
        approx_z = batch_mm(update, approx_z)
    root_inv = approx_z / jnp.sqrt(bound_norm)[:, None, None]
    inner = jnp.einsum("bij,bj->bi", root_inv, forcing, precision=lax.Precision.HIGHEST)
    mean_weights = jnp.einsum("bij,bj->bi", root_inv, inner, precision=lax.Precision.HIGHEST)
    mixing = (
        jnp.sqrt(jnp.float32(ensemble_size - 1)) * root_inv + mean_weights[:, :, None] - identity
    )
    increment = jnp.einsum("bjc,bjk->kbc", deviation, mixing, precision=lax.Precision.HIGHEST)
    return increment.astype(jnp.bfloat16)


def on_device(ensemble, obs_cell, obs_count, obs_value, obs_rinv):
    groups = lax.axis_size("mem")
    local_members = ensemble.shape[0]
    blocks = obs_cell.shape[1]
    cell_width = ensemble.shape[1] // (groups * blocks)
    pieces = ensemble.reshape(local_members, groups, blocks, cell_width)
    arrived = lax.all_to_all(pieces, "mem", split_axis=1, concat_axis=0, tiled=True)
    deviation, average = center_blocks(arrived[:, 0])
    obs_rows = observe(deviation, average, obs_cell[0], obs_count[0], obs_value[0], obs_rinv[0])
    padded_rows = with_halo(obs_rows, (("mem", 0),), 1)
    padded = gram_of(padded_rows)
    localized = padded[1:-1] + localize * (padded[:-2] + padded[2:])
    increment = transform_apply(localized, deviation)
    ensemble_size = increment.shape[0]
    outgoing = increment.reshape(ensemble_size, 1, blocks * cell_width)
    returned = lax.all_to_all(outgoing, "mem", split_axis=0, concat_axis=1, tiled=True)
    return returned.reshape(local_members, groups * blocks * cell_width)


def by_shape(ensemble, *observations):
    groups = lax.axis_size("mem")
    local, cells = ensemble.shape
    blocks, slots = observations[0].shape[1:]
    width = cells // (groups * blocks)
    aligned = local % 16 == 0 and width % 128 == 0 and slots % 128 == 0
    aligned = aligned and (groups * local) % 128 == 0 and groups > 1 and blocks > 2 and blocks % 2 == 0
    return (fused if aligned else on_device)(ensemble, *observations)


def solution(mesh):
    placed = (
        P("mem", "blk"),
        P("blk", "mem", None),
        P("blk", "mem"),
        P("blk", "mem", None),
        P("blk", "mem", None),
    )
    return jax.shard_map(
        by_shape, mesh=mesh, in_specs=placed, out_specs=P("mem", "blk"), check_vma=False
    )
```
